32 devices in a mesh: data: 4 (over z), model: 8 (over y, x, core).
Axes of the slice: x: 2, y: 2, z: 4, core: 2. Of those that a mesh axis runs over, the one named last changes fastest.
Arguments:
- hidden: bfloat16 [8192, 3072], P('data', 'model')
- unembed: bfloat16 [128256, 3072], P('model', 'data')
- draft_ids: int32 [8192], P('data')
- q_prob: float32 [8192], P('data')
Outputs:
- output 1: float32 [8192], P('data')
- output 2: float32 [8192], P('data')
All inputs are finite; a program needn't handle non-finite values.
Results may differ from the reference program's by a relative error of at most 0.001.
Values are sent between devices in bfloat16 or wider.
A program may use at most 1 GiB of HBM per device.

```python
import math
import jax
import jax.numpy as jnp
from jax import lax

VOCAB = 128256
WIDTH = 3072
ROWS = 8192
ROW_BLOCK = 64


def setup_inputs(seed: int = 0) -> dict:
    base_key = jax.random.key(seed)
    k_hid, k_wt, k_draft, k_prob = jax.random.split(base_key, 4)
    hidden = jax.random.normal(k_hid, (ROWS, WIDTH), jnp.float32).astype(jnp.bfloat16)
    unembed = (jax.random.normal(k_wt, (VOCAB, WIDTH), jnp.float32) * WIDTH ** -0.5).astype(jnp.bfloat16)
    draft_ids = jax.random.randint(k_draft, (ROWS,), 0, VOCAB, jnp.int32).at[0].set(VOCAB - 1)
    log_q = -math.log(VOCAB) - 0.5 + jax.random.uniform(k_prob, (ROWS,), jnp.float32, -1.0, 1.0)
    q_prob = jnp.exp(log_q)
    return {"hidden": hidden, "unembed": unembed, "draft_ids": draft_ids, "q_prob": q_prob}


def reference(hidden, unembed, draft_ids, q_prob):
    blocks = ROWS // ROW_BLOCK
    vocab_ids = jnp.arange(VOCAB, dtype=jnp.int32)[None, :]

    def one_block(block_in):
        h_blk, d_blk = block_in
        logits = jnp.dot(h_blk, unembed.T, preferred_element_type=jnp.float32)
        row_max = jnp.max(logits, axis=1)
        log_sum = row_max + jnp.log(jnp.sum(jnp.exp(logits - row_max[:, None]), axis=1))
        picked = jnp.sum(jnp.where(vocab_ids == d_blk[:, None], logits, 0.0), axis=1)
        return picked - log_sum

    log_prob = lax.map(one_block, (hidden.reshape(blocks, ROW_BLOCK, WIDTH), draft_ids.reshape(blocks, ROW_BLOCK))).reshape(ROWS)
    accept = jnp.minimum(1.0, jnp.exp(log_prob) / q_prob)
    return log_prob, accept
```

```python
import functools

import jax
import jax.numpy as jnp
from jax import lax
from jax.experimental import pallas as pl
from jax.experimental.pallas import tpu as pltpu
from jax.sharding import PartitionSpec as P

MESH = pl.DeviceIdType.MESH
NZ = 4
NM = 8
OFFSETS = (-1, 1, -2, 2, -3, 3)
BLOCK = 256


def chunk_plan(piece, big, tails):
    count = (piece - sum(tails)) // big
    assert count * big + sum(tails) == piece
    starts, at = [], count * big
    for size in tails:
        starts.append((at, size))
        at += size
    return count, starts


def kernel(
    cfg, h_ref, w_ref, draft_ref, stats_ref, land_ref,
    hv, wb, dv, m_acc, s_acc, p_acc,
    loc_sem, dr_s, dr_r, hz_s, hz_r, hx_s, hx_r, hy_s, hy_r, dx_s, dx_r, dy_s, dy_r, hp_s, hp_r, w_s, w_r, ld_sem,
):
    slab, part, piece, step, shard, width, big, count, tails = cfg
    d = lax.axis_index("data")
    m = lax.axis_index("model")
    xn = m + 2 - 4 * ((m // 2) % 2)
    yn = m + 4 - 8 * (m // 4)
    xy = xn + 4 - 8 * (xn // 4)
    pn = m + 1 - 2 * (m % 2)

    barrier = pltpu.get_barrier_semaphore()
    for j in (1, 2, 3):
        pl.semaphore_signal(barrier, inc=1, device_id=(lax.rem(d + j, NZ), m), device_id_type=MESH)
    for other in (xn, yn, pn):
        pl.semaphore_signal(barrier, inc=1, device_id=(d, other), device_id_type=MESH)
    pl.semaphore_wait(barrier, 6)

    def spot(s, mm):
        return hv.at[pl.ds(pl.multiple_of(s * slab, slab), slab), pl.ds(pl.multiple_of(mm * part, part), part)]

    def half(s, mm, which):
        rows = slab // 2
        return hv.at[pl.ds(pl.multiple_of(s * slab + which * rows, rows), rows), pl.ds(pl.multiple_of(mm * part, part), part)]

    def remote(src, dst, ssem, rsem, to):
        return pltpu.make_async_remote_copy(src_ref=src, dst_ref=dst, send_sem=ssem, recv_sem=rsem, device_id=to, device_id_type=MESH)

    def piece_start(t):
        return step * t + (piece - step) * (t // 3)

    def w_copy(j, idx, c0, size):
        t = lax.rem(d + j, NZ)
        return remote(
            w_ref.at[pl.ds(pl.multiple_of(piece_start(t) + c0, 16), size), :],
            land_ref.at[pl.ds(pl.multiple_of(c0, 16), size), pl.ds(pl.multiple_of(d * width, width), width)],
            w_s.at[j - 1, idx], w_r.at[j - 1, idx], (t, m),
        )

    def hz_copy(src, s, ssem, to):
        return remote(src, spot(s, m), ssem, hz_r.at[s], (to, m))

    def hx_copy(src, s):
        return remote(src, spot(s, m), hx_s.at[s], hx_r.at[s], (d, xn))

    def hy_copy(src, s):
        return remote(src, spot(s, m), hy_s.at[s], hy_r.at[s], (d, yn))

    def dx_copy(s):
        return remote(half(s, yn, 0), half(s, yn, 0), dx_s.at[s], dx_r.at[s], (d, xn))

    def dy_copy(s):
        return remote(half(s, xn, 1), half(s, xn, 1), dy_s.at[s], dy_r.at[s], (d, yn))

    def hp_copy(src, s, mm, k):
        return remote(src, spot(s, mm), hp_s.at[s, k], hp_r.at[s, k], (d, pn))

    own = pltpu.make_async_copy(h_ref, spot(d, m), loc_sem.at[0])
    own.start()
    own_draft = pltpu.make_async_copy(draft_ref, dv.at[d], loc_sem.at[1])
    own_draft.start()

    @pl.when(d < NZ - 1)
    def _():
        hz_copy(h_ref, d, hz_s.at[d], d + 1).start()

    @pl.when(d > 0)
    def _():
        hz_copy(h_ref, d, hz_s.at[NZ], d - 1).start()

    hx_copy(h_ref, d).start()
    hy_copy(h_ref, d).start()
    hp_copy(h_ref, d, m, 0).start()
    drafts = [
        remote(draft_ref, dv.at[d], dr_s.at[j - 1], dr_r.at[j - 1], (lax.rem(d + j, NZ), m)) for j in (1, 2, 3)
    ]
    for copy in drafts:
        copy.start()

    spans = [(c * big, big) for c in range(count)] + list(tails)

    def send_weights(lo, hi):
        for idx in range(lo, hi):
            for j in (2, 1, 3):
                w_copy(j, idx, *spans[idx]).start()

    for o in OFFSETS:
        s = d + o

        @pl.when((s >= 0) & (s < NZ))
        def _(o=o, s=s):
            src = spot(s, m)
            hz_copy(src, s, hz_s.at[s], d + (1 if o < 0 else -1)).wait_recv()
            if o < 0:
                @pl.when(d < NZ - 1)
                def _():
                    hz_copy(src, s, hz_s.at[s], d + 1).start()
            else:
                @pl.when(d > 0)
                def _():
                    hz_copy(src, s, hz_s.at[s], d - 1).start()
            hx_copy(src, s).start()
            hy_copy(src, s).start()
            hp_copy(src, s, m, 0).start()

        if o == 1:
            send_weights(0, 1)
        if o == 2:
            send_weights(1, len(spans))

    for o in (0,) + OFFSETS:
        s = d + o

        @pl.when((s >= 0) & (s < NZ))
        def _(s=s):
            hx_copy(spot(s, m), s).wait_recv()
            dy_copy(s).start()
            hp_copy(spot(s, xn), s, xn, 1).start()
            hy_copy(spot(s, m), s).wait_recv()
            dx_copy(s).start()
            hp_copy(spot(s, yn), s, yn, 2).start()

    for o in (0,) + OFFSETS:
        s = d + o

        @pl.when((s >= 0) & (s < NZ))
        def _(s=s):
            dx_copy(s).wait_recv()
            dy_copy(s).wait_recv()
            hp_copy(spot(s, xy), s, xy, 3).start()

    m_acc[...] = jnp.full(m_acc.shape, -jnp.inf, jnp.float32)
    s_acc[...] = jnp.zeros_like(s_acc)
    p_acc[...] = jnp.zeros_like(p_acc)

    own.wait()
    own_draft.wait()
    for copy in drafts:
        copy.wait()
    for s in range(NZ):
        for k in range(4):
            hp_copy(spot(s, m), s, m, k).wait_recv()

    base = m * shard + piece_start(d)
    limit = step + (piece - step) * (d // 2)

    def work(idx, c0, size, last):
        loads = [
            pltpu.make_async_copy(
                w_ref.at[pl.ds(pl.multiple_of(piece_start(d) + c0, 16), size), :],
                wb.at[pl.ds(0, size), pl.ds(pl.multiple_of(d * width, width), width)],
                ld_sem.at[0],
            )
        ]
        loads[0].start()
        for j in (1, 2, 3):
            w_copy(j, idx, c0, size).wait_recv()
            cols = pl.ds(pl.multiple_of(lax.rem(d + NZ - j, NZ) * width, width), width)
            copy = pltpu.make_async_copy(
                land_ref.at[pl.ds(pl.multiple_of(c0, 16), size), cols], wb.at[pl.ds(0, size), cols], ld_sem.at[j]
            )
            copy.start()
            loads.append(copy)
        for copy in loads:
            copy.wait()

        per = slab // BLOCK

        def block(n, carry):
            rows = pl.multiple_of(n * BLOCK, BLOCK)
            logits = lax.dot_general(
                wb[pl.ds(0, size), :], hv[pl.ds(rows, BLOCK), :], (((1,), (1,)), ((), ())),
                preferred_element_type=jnp.float32,
            )
            tiles = logits.reshape(size // 8, 8, BLOCK)
            ids = 8 * lax.broadcasted_iota(jnp.int32, tiles.shape, 0) + lax.broadcasted_iota(jnp.int32, tiles.shape, 1)
            want = dv[n // per, :, pl.ds(pl.multiple_of((n % per) * BLOCK, BLOCK), BLOCK)] - (base + c0)
            if last:
                tiles = jnp.where(ids < limit - c0, tiles, -jnp.inf)
                want = jnp.where(want < limit - c0, want, -1)
            cols = pl.ds(rows, BLOCK)
            old = m_acc[:, cols]
            new = jnp.maximum(old, jnp.max(tiles, axis=0))
            m_acc[:, cols] = new
            s_acc[:, cols] = s_acc[:, cols] * jnp.exp(old - new) + jnp.sum(jnp.exp(tiles - new[None]), axis=0)
            p_acc[:, cols] = p_acc[:, cols] + jnp.sum(jnp.where(ids == want[None], tiles, 0.0), axis=0)
            return carry

        lax.fori_loop(0, NZ * per, block, 0)

    def big_chunk(c, carry):
        work(c, c * big, big, False)
        return carry

    lax.fori_loop(0, count, big_chunk, 0)
    for k, (c0, size) in enumerate(tails):
        work(count + k, c0, size, k == len(tails) - 1)

    top = jnp.max(m_acc[...], axis=0, keepdims=True)
    stats_ref[0:1, :] = top
    stats_ref[1:2, :] = jnp.sum(s_acc[...] * jnp.exp(m_acc[...] - top), axis=0, keepdims=True)
    stats_ref[2:3, :] = jnp.sum(p_acc[...], axis=0, keepdims=True)

    for idx, span in enumerate(spans):
        for j in (1, 2, 3):
            w_copy(j, idx, *span).wait_send()

    @pl.when(d < NZ - 1)
    def _():
        hz_copy(h_ref, d, hz_s.at[d], d + 1).wait_send()

    @pl.when(d > 0)
    def _():
        hz_copy(h_ref, d, hz_s.at[NZ], d - 1).wait_send()

    for o in OFFSETS:
        s = d + o
        on = (s >= 0) & (d < NZ - 1) if o < 0 else (s < NZ) & (d > 0)

        @pl.when(on)
        def _(o=o, s=s):
            hz_copy(spot(s, m), s, hz_s.at[s], d + (1 if o < 0 else -1)).wait_send()

    for s in range(NZ):
        hx_copy(spot(s, m), s).wait_send()
        hy_copy(spot(s, m), s).wait_send()
        dx_copy(s).wait_send()
        dy_copy(s).wait_send()
        for k in range(4):
            hp_copy(spot(s, m), s, m, k).wait_send()


def solution(mesh):
    def per_device(h_part, w_part, draft_loc, q_loc):
        slab, part = h_part.shape
        shard, width = w_part.shape
        rows, full = slab * NZ, part * NM
        step = shard // NZ // 16 * 16
        piece = shard - 3 * step - ((shard - 3 * step) - step) // 2
        big = 512
        tails = (256, piece - 256 - (piece - 256 - 160) // big * big)
        count, tail_spans = chunk_plan(piece, big, tails)
        n_chunks = count + len(tails)
        cfg = (slab, part, piece, step, shard, width, big, count, tuple(tail_spans))
        dma = pltpu.SemaphoreType.DMA
        stats, _ = pl.pallas_call(
            functools.partial(kernel, cfg),
            out_shape=(
                jax.ShapeDtypeStruct((3, rows), jnp.float32),
                jax.ShapeDtypeStruct((piece, full), jnp.bfloat16),
            ),
            in_specs=[pl.BlockSpec(memory_space=pl.ANY)] * 3,
            out_specs=(pl.BlockSpec(memory_space=pltpu.VMEM), pl.BlockSpec(memory_space=pl.ANY)),
            scratch_shapes=[
                pltpu.VMEM((rows, full), jnp.bfloat16),
                pltpu.VMEM((big, full), jnp.bfloat16),
                pltpu.VMEM((NZ, 1, slab), jnp.int32),
                pltpu.VMEM((8, rows), jnp.float32),
                pltpu.VMEM((8, rows), jnp.float32),
                pltpu.VMEM((8, rows), jnp.float32),
                dma((2,)), dma((3,)), dma((3,)), dma((NZ + 1,)), dma((NZ,)),
                dma((NZ,)), dma((NZ,)), dma((NZ,)), dma((NZ,)),
                dma((NZ,)), dma((NZ,)), dma((NZ,)), dma((NZ,)),
                dma((NZ, 4)), dma((NZ, 4)), dma((3, n_chunks)), dma((3, n_chunks)), dma((4,)),
            ],
            compiler_params=pltpu.CompilerParams(
                collective_id=0, has_side_effects=True, vmem_limit_bytes=67043328
            ),
        )(h_part, w_part, draft_loc.reshape(1, slab))

        mine = lax.all_to_all(stats.reshape(3, NZ, slab).swapaxes(0, 1), "data", 0, 0)
        top = jnp.max(mine[:, 0], axis=0)
        total = jnp.sum(mine[:, 1] * jnp.exp(mine[:, 0] - top), axis=0)
        both = lax.all_gather(jnp.stack([top, total, jnp.sum(mine[:, 2], axis=0)]), "model", axis=0)
        row_max = jnp.max(both[:, 0], axis=0)
        row_sum = jnp.sum(both[:, 1] * jnp.exp(both[:, 0] - row_max), axis=0)
        log_prob = jnp.sum(both[:, 2], axis=0) - row_max - jnp.log(row_sum)
        accept = jnp.minimum(1.0, jnp.exp(log_prob) / q_loc)
        return log_prob, accept

    return jax.shard_map(per_device, mesh=mesh, in_specs=(P("data", "model"), P("model", "data"), P("data"), P("data")), out_specs=(P("data"), P("data")), check_vma=False)
```

```python
import functools

import jax
import jax.numpy as jnp
from jax import lax
from jax.experimental import pallas as pl
from jax.experimental.pallas import tpu as pltpu
from jax.sharding import PartitionSpec as P

MESH = pl.DeviceIdType.MESH
NZ = 4
NM = 8
OFFSETS = (-1, 1, -2, 2, -3, 3)
BLOCK = 512
BIG = 288
AHEAD = 13


def merge(shares):
    shares = [jnp.split(s, 3, axis=1) for s in shares]
    top = functools.reduce(jnp.maximum, [s[0] for s in shares])
    return top, sum(s[1] * jnp.exp(s[0] - top) for s in shares), sum(s[2] for s in shares)


def kernel(
    cfg, h_ref, w_ref, draft_ref, q_ref, logp_ref, accept_ref, land_ref,
    hv, wb, dv, m_acc, s_acc, p_acc, even, odd, part_acc, stats, zin, gat,
    zx_s, zx_r, mx_s, mx_r, loc_sem, dr_s, dr_r, hz_s, hz_r, hx_s, hx_r, hy_s, hy_r, dx_s, dx_r, dy_s, dy_r, hp_s, hp_r, w_s, w_r, ld_sem,
):
    slab, part, piece, step, shard, width, big, count = cfg
    tail = piece - count * big
    d = lax.axis_index("data")
    m = lax.axis_index("model")
    xn = m + 2 - 4 * ((m // 2) % 2)
    yn = m + 4 - 8 * (m // 4)
    xy = xn + 4 - 8 * (xn // 4)
    pn = m + 1 - 2 * (m % 2)

    barrier = pltpu.get_barrier_semaphore()
    for j in (1, 2, 3):
        pl.semaphore_signal(barrier, inc=1, device_id=(lax.rem(d + j, NZ), m), device_id_type=MESH)
    for k in range(1, NM):
        pl.semaphore_signal(barrier, inc=1, device_id=(d, lax.rem(m + k, NM)), device_id_type=MESH)
    pl.semaphore_wait(barrier, NZ - 1 + NM - 1)

    def spot(s, mm):
        return hv.at[pl.ds(pl.multiple_of(s * slab, slab), slab), pl.ds(pl.multiple_of(mm * part, part), part)]

    def half(s, mm, which):
        rows = slab // 2
        return hv.at[pl.ds(pl.multiple_of(s * slab + which * rows, rows), rows), pl.ds(pl.multiple_of(mm * part, part), part)]

    def remote(src, dst, ssem, rsem, to):
        return pltpu.make_async_remote_copy(src_ref=src, dst_ref=dst, send_sem=ssem, recv_sem=rsem, device_id=to, device_id_type=MESH)

    def piece_start(t):
        return step * t + (piece - step) * (t // 3)

    def w_copy(j, idx, c0, size):
        t = lax.rem(d + j, NZ)
        return remote(
            w_ref.at[pl.ds(pl.multiple_of(piece_start(t) + c0, 16), size), :],
            land_ref.at[pl.ds(pl.multiple_of(c0, 16), size), pl.ds(pl.multiple_of(d * width, width), width)],
            w_s.at[j - 1, idx], w_r.at[j - 1, idx], (t, m),
        )

    def hz_copy(src, s, ssem, to):
        return remote(src, spot(s, m), ssem, hz_r.at[s], (to, m))

    def hx_copy(src, s):
        return remote(src, spot(s, m), hx_s.at[s], hx_r.at[s], (d, xn))

    def hy_copy(src, s):
        return remote(src, spot(s, m), hy_s.at[s], hy_r.at[s], (d, yn))

    def dx_copy(s):
        return remote(half(s, yn, 0), half(s, yn, 0), dx_s.at[s], dx_r.at[s], (d, xn))

    def dy_copy(s):
        return remote(half(s, xn, 1), half(s, xn, 1), dy_s.at[s], dy_r.at[s], (d, yn))

    def hp_copy(src, s, mm, k):
        return remote(src, spot(s, mm), hp_s.at[s, k], hp_r.at[s, k], (d, pn))

    own = pltpu.make_async_copy(h_ref, spot(d, m), loc_sem.at[0])
    own.start()
    own_draft = pltpu.make_async_copy(draft_ref, dv.at[d], loc_sem.at[1])
    own_draft.start()

    @pl.when(d < NZ - 1)
    def _():
        hz_copy(h_ref, d, hz_s.at[d], d + 1).start()

    @pl.when(d > 0)
    def _():
        hz_copy(h_ref, d, hz_s.at[NZ], d - 1).start()

    hx_copy(h_ref, d).start()
    hy_copy(h_ref, d).start()
    hp_copy(h_ref, d, m, 0).start()
    drafts = [
        remote(draft_ref, dv.at[d], dr_s.at[j - 1], dr_r.at[j - 1], (lax.rem(d + j, NZ), m)) for j in (1, 2, 3)
    ]
    for copy in drafts:
        copy.start()

    spans = [(c * big, big) for c in range(count)] + [(count * big, tail)]
    to_near, from_near = 1 + 2 * (d % 2), 3 - 2 * (d % 2)

    def send_weights(lo, hi):
        for idx in range(lo, hi):
            for j in (2, 1, 3):
                w_copy(j, idx, *spans[idx]).start()

    for o in OFFSETS:
        s = d + o

        @pl.when((s >= 0) & (s < NZ))
        def _(o=o, s=s):
            src = spot(s, m)
            hz_copy(src, s, hz_s.at[s], d + (1 if o < 0 else -1)).wait_recv()
            if o < 0:
                @pl.when(d < NZ - 1)
                def _():
                    hz_copy(src, s, hz_s.at[s], d + 1).start()
            else:
                @pl.when(d > 0)
                def _():
                    hz_copy(src, s, hz_s.at[s], d - 1).start()
            hx_copy(src, s).start()
            hy_copy(src, s).start()
            hp_copy(src, s, m, 0).start()

        if o == 1:
            send_weights(0, 1)
            w_copy(to_near, count, *spans[count]).start()
        if o == 2:
            send_weights(1, AHEAD)

    for o in (0,) + OFFSETS:
        s = d + o

        @pl.when((s >= 0) & (s < NZ))
        def _(s=s):
            hx_copy(spot(s, m), s).wait_recv()
            dy_copy(s).start()
            hp_copy(spot(s, xn), s, xn, 1).start()
            hy_copy(spot(s, m), s).wait_recv()
            dx_copy(s).start()
            hp_copy(spot(s, yn), s, yn, 2).start()

    for o in (0,) + OFFSETS:
        s = d + o

        @pl.when((s >= 0) & (s < NZ))
        def _(s=s):
            dx_copy(s).wait_recv()
            dy_copy(s).wait_recv()
            hp_copy(spot(s, xy), s, xy, 3).start()

    m_acc[...] = jnp.full(m_acc.shape, -jnp.inf, jnp.float32)
    s_acc[...] = jnp.zeros_like(s_acc)
    p_acc[...] = jnp.zeros_like(p_acc)

    own.wait()
    own_draft.wait()
    for copy in drafts:
        copy.wait()
    for s in range(NZ):
        for k in range(4):
            hp_copy(spot(s, m), s, m, k).wait_recv()

    base = m * shard + piece_start(d)
    limit = step + (piece - step) * (d // 2)

    per = slab // BLOCK
    blocks = NZ * per
    hw = 2 * width
    near = pl.ds(pl.multiple_of(d // 2 * hw, hw), hw)
    far = pl.ds(pl.multiple_of((1 - d // 2) * hw, hw), hw)

    def load(src, c0, size, cols, k):
        return pltpu.make_async_copy(src.at[pl.ds(pl.multiple_of(c0, 16), size), cols], wb.at[pl.ds(0, size), cols], ld_sem.at[k])

    def load_own(c0, size):
        cols = pl.ds(pl.multiple_of(d * width, width), width)
        return pltpu.make_async_copy(
            w_ref.at[pl.ds(pl.multiple_of(piece_start(d) + c0, 16), size), :], wb.at[pl.ds(0, size), cols], ld_sem.at[0]
        )

    def column(j):
        return pl.ds(pl.multiple_of(lax.rem(d + NZ - j, NZ) * width, width), width)

    def block_of(n):
        return pl.ds(pl.multiple_of(n * BLOCK, BLOCK), BLOCK)

    def product(n, size, cols):
        return lax.dot_general(
            wb[pl.ds(0, size), cols], hv[block_of(n), cols], (((1,), (1,)), ((), ())), preferred_element_type=jnp.float32
        )

    def fold(n, c0, size, ref, last):
        cols = block_of(n)
        tiles = ref[pl.ds(0, size), :].reshape(size // 8, 8, BLOCK)
        ids = 8 * lax.broadcasted_iota(jnp.int32, tiles.shape, 0) + lax.broadcasted_iota(jnp.int32, tiles.shape, 1)
        want = dv[n // per, :, pl.ds(pl.multiple_of((n % per) * BLOCK, BLOCK), BLOCK)] - (base + c0)
        if last:
            tiles = jnp.where(ids < limit - c0, tiles, -jnp.inf)
            want = jnp.where(want < limit - c0, want, -1)
        old = m_acc[:, cols]
        new = jnp.maximum(old, jnp.max(tiles, axis=0))
        m_acc[:, cols] = new
        s_acc[:, cols] = s_acc[:, cols] * jnp.exp(old - new) + jnp.sum(jnp.exp(tiles - new[None]), axis=0)
        p_acc[:, cols] = p_acc[:, cols] + jnp.sum(jnp.where(ids == want[None], tiles, 0.0), axis=0)

    def sweep(c0, size, fill, last):
        def pair(n, carry):
            fill(2 * n + 1, odd)
            fold(2 * n, c0, size, even, last)
            fill(2 * n + 2, even)
            fold(2 * n + 1, c0, size, odd, last)
            return carry

        fill(0, even)
        lax.fori_loop(0, blocks // 2 - 1, pair, 0)
        fill(blocks - 1, odd)
        fold(blocks - 2, c0, size, even, last)
        fold(blocks - 1, c0, size, odd, last)

    t0 = count * big
    loads = [load_own(t0, tail), load(land_ref, t0, tail, column(from_near), 1)]
    w_copy(from_near, count, t0, tail).wait_recv()
    for copy in loads:
        copy.start()
    for copy in loads:
        copy.wait()

    def first_half(n, carry):
        part_acc[:, block_of(n)] = product(n, tail, near)
        return carry

    lax.fori_loop(0, blocks, first_half, 0)

    def big_chunk(c, carry):
        c0 = c * big
        loads = [load_own(c0, big)]
        loads[0].start()
        for j in (1, 2, 3):
            w_copy(j, c, c0, big).wait_recv()
            loads.append(load(land_ref, c0, big, column(j), j))
            loads[-1].start()
        ahead = c + AHEAD

        @pl.when(ahead < count)
        def _():
            for j in (2, 1, 3):
                w_copy(j, ahead, ahead * big, big).start()

        @pl.when(ahead == count)
        def _():
            for j in (2, from_near):
                w_copy(j, count, t0, tail).start()

        for copy in loads:
            copy.wait()

        def fill(n, ref):
            ref[...] = product(n, big, slice(None))

        sweep(c0, big, fill, False)
        return carry

    lax.fori_loop(0, count, big_chunk, 0)

    for j in (2, to_near):
        w_copy(j, count, t0, tail).wait_recv()
    rest = load(land_ref, t0, tail, far, 1)
    rest.start()
    rest.wait()

    def fill_rest(n, ref):
        ref[pl.ds(0, tail), :] = part_acc[:, block_of(n)] + product(n, tail, far)

    sweep(t0, tail, fill_rest, True)

    def put(ref, at, *share):
        for k, value in enumerate(share):
            ref[at, :, pl.ds(k * slab, slab)] = value

    for t in range(NZ):
        cols = pl.ds(t * slab, slab)
        tops = m_acc[:, cols]
        top = jnp.max(tops, axis=0, keepdims=True)
        put(stats, t, top, jnp.sum(s_acc[:, cols] * jnp.exp(tops - top), axis=0, keepdims=True), jnp.sum(p_acc[:, cols], axis=0, keepdims=True))

    for idx, span in enumerate(spans):
        for j in (1, 2, 3):
            w_copy(j, idx, *span).wait_send()

    @pl.when(d < NZ - 1)
    def _():
        hz_copy(h_ref, d, hz_s.at[d], d + 1).wait_send()

    @pl.when(d > 0)
    def _():
        hz_copy(h_ref, d, hz_s.at[NZ], d - 1).wait_send()

    for o in OFFSETS:
        s = d + o
        on = (s >= 0) & (d < NZ - 1) if o < 0 else (s < NZ) & (d > 0)

        @pl.when(on)
        def _(o=o, s=s):
            hz_copy(spot(s, m), s, hz_s.at[s], d + (1 if o < 0 else -1)).wait_send()

    for s in range(NZ):
        hx_copy(spot(s, m), s).wait_send()
        hy_copy(spot(s, m), s).wait_send()
        dx_copy(s).wait_send()
        dy_copy(s).wait_send()
        for k in range(4):
            hp_copy(spot(s, m), s, m, k).wait_send()

    def zx_copy(j):
        t = lax.rem(d + j, NZ)
        return remote(stats.at[t], zin.at[j - 1], zx_s.at[j - 1], zx_r.at[j - 1], (t, m))

    def mx_copy(k):
        return remote(gat.at[m], gat.at[m], mx_s.at[k - 1], mx_r.at[k - 1], (d, lax.rem(m + k, NM)))

    for j in (2, 1, 3):
        zx_copy(j).start()
    for j in (1, 2, 3):
        zx_copy(j).wait()
    shares = [stats[d]] + [zin[j] for j in range(NZ - 1)]
    put(gat, m, *merge(shares))
    for k in range(1, NM):
        mx_copy(k).start()
    for k in range(1, NM):
        mx_copy(k).wait()
    top, total, picked = merge([gat[k] for k in range(NM)])
    log_prob = picked - top - jnp.log(total)
    logp_ref[...] = log_prob
    accept_ref[...] = jnp.minimum(1.0, jnp.exp(log_prob) / q_ref[...])


def solution(mesh):
    def per_device(h_part, w_part, draft_loc, q_loc):
        slab, part = h_part.shape
        shard, width = w_part.shape
        rows, full = slab * NZ, part * NM
        step = shard // NZ // 16 * 16
        piece = shard - 3 * step - ((shard - 3 * step) - step) // 2
        big, count = BIG, (piece - 1) // BIG
        n_chunks = count + 1
        cfg = (slab, part, piece, step, shard, width, big, count)
        dma = pltpu.SemaphoreType.DMA
        log_prob, accept, _ = pl.pallas_call(
            functools.partial(kernel, cfg),
            out_shape=(
                jax.ShapeDtypeStruct((1, slab), jnp.float32),
                jax.ShapeDtypeStruct((1, slab), jnp.float32),
                jax.ShapeDtypeStruct((piece, full), jnp.bfloat16),
            ),
            in_specs=[pl.BlockSpec(memory_space=pl.ANY)] * 3 + [pl.BlockSpec(memory_space=pltpu.VMEM)],
            out_specs=(
                pl.BlockSpec(memory_space=pltpu.VMEM),
                pl.BlockSpec(memory_space=pltpu.VMEM),
                pl.BlockSpec(memory_space=pl.ANY),
            ),
            scratch_shapes=[
                pltpu.VMEM((rows, full), jnp.bfloat16),
                pltpu.VMEM((big, full), jnp.bfloat16),
                pltpu.VMEM((NZ, 1, slab), jnp.int32),
                pltpu.VMEM((8, rows), jnp.float32),
                pltpu.VMEM((8, rows), jnp.float32),
                pltpu.VMEM((8, rows), jnp.float32),
                pltpu.VMEM((big, BLOCK), jnp.float32),
                pltpu.VMEM((big, BLOCK), jnp.float32),
                pltpu.VMEM((piece - count * big, rows), jnp.float32),
                pltpu.VMEM((NZ, 1, 3 * slab), jnp.float32),
                pltpu.VMEM((NZ - 1, 1, 3 * slab), jnp.float32),
                pltpu.VMEM((NM, 1, 3 * slab), jnp.float32),
                dma((NZ - 1,)), dma((NZ - 1,)), dma((NM - 1,)), dma((NM - 1,)),
                dma((2,)), dma((3,)), dma((3,)), dma((NZ + 1,)), dma((NZ,)),
                dma((NZ,)), dma((NZ,)), dma((NZ,)), dma((NZ,)),
                dma((NZ,)), dma((NZ,)), dma((NZ,)), dma((NZ,)),
                dma((NZ, 4)), dma((NZ, 4)), dma((3, n_chunks)), dma((3, n_chunks)), dma((4,)),
            ],
            compiler_params=pltpu.CompilerParams(
                collective_id=0, has_side_effects=True, vmem_limit_bytes=67043328
            ),
        )(h_part, w_part, draft_loc.reshape(1, slab), q_loc.reshape(1, slab))
        return log_prob.reshape(slab), accept.reshape(slab)

    return jax.shard_map(per_device, mesh=mesh, in_specs=(P("data", "model"), P("model", "data"), P("data"), P("data")), out_specs=(P("data"), P("data")), check_vma=False)
```

```python
import functools

import jax
import jax.numpy as jnp
from jax import lax
from jax.experimental import pallas as pl
from jax.experimental.pallas import tpu as pltpu
from jax.sharding import PartitionSpec as P

MESH = pl.DeviceIdType.MESH
NZ = 4
NM = 8
OFFSETS = (-1, 1, -2, 2, -3, 3)
BLOCK = 512
BIG = 288
LATE = 2


def merge(shares):
    shares = [jnp.split(s, 2, axis=1) for s in shares]
    top = functools.reduce(jnp.maximum, [s[0] for s in shares])
    return top + jnp.log(sum(jnp.exp(s[0] - top) for s in shares)), sum(s[1] for s in shares)


def kernel(
    cfg, h_ref, w_ref, draft_ref, q_ref, logp_ref, accept_ref, land_ref,
    hv, wb, dv, m_acc, s_acc, p_acc, even, odd, part_acc, stats, zin, gat,
    zx_s, zx_r, mx_s, mx_r, loc_sem, dr_s, dr_r, hz_s, hz_r, hx_s, hx_r, hy_s, hy_r, dx_s, dx_r, dy_s, dy_r, hp_s, hp_r, w_s, w_r, ld_sem,
):
    slab, part, piece, step, shard, width, big, count = cfg
    tail = piece - count * big
    d = lax.axis_index("data")
    m = lax.axis_index("model")
    xn = m + 2 - 4 * ((m // 2) % 2)
    yn = m + 4 - 8 * (m // 4)
    xy = xn + 4 - 8 * (xn // 4)
    pn = m + 1 - 2 * (m % 2)

    barrier = pltpu.get_barrier_semaphore()
    for j in (1, 2, 3):
        pl.semaphore_signal(barrier, inc=1, device_id=(lax.rem(d + j, NZ), m), device_id_type=MESH)
    for k in range(1, NM):
        pl.semaphore_signal(barrier, inc=1, device_id=(d, lax.rem(m + k, NM)), device_id_type=MESH)
    pl.semaphore_wait(barrier, NZ - 1 + NM - 1)

    def spot(s, mm):
        return hv.at[pl.ds(pl.multiple_of(s * slab, slab), slab), pl.ds(pl.multiple_of(mm * part, part), part)]

    def half(s, mm, which):
        rows = slab // 2
        return hv.at[pl.ds(pl.multiple_of(s * slab + which * rows, rows), rows), pl.ds(pl.multiple_of(mm * part, part), part)]

    def remote(src, dst, ssem, rsem, to):
        return pltpu.make_async_remote_copy(src_ref=src, dst_ref=dst, send_sem=ssem, recv_sem=rsem, device_id=to, device_id_type=MESH)

    def piece_start(t):
        return step * t + (piece - step) * (t // 3)

    def w_copy(j, idx, c0, size):
        t = lax.rem(d + j, NZ)
        return remote(
            w_ref.at[pl.ds(pl.multiple_of(piece_start(t) + c0, 16), size), :],
            land_ref.at[pl.ds(pl.multiple_of(c0, 16), size), pl.ds(pl.multiple_of(d * width, width), width)],
            w_s.at[j - 1, idx], w_r.at[j - 1, idx], (t, m),
        )

    def hz_copy(src, s, ssem, to):
        return remote(src, spot(s, m), ssem, hz_r.at[s], (to, m))

    def hx_copy(src, s):
        return remote(src, spot(s, m), hx_s.at[s], hx_r.at[s], (d, xn))

    def hy_copy(src, s):
        return remote(src, spot(s, m), hy_s.at[s], hy_r.at[s], (d, yn))

    def dx_copy(s):
        return remote(half(s, yn, 0), half(s, yn, 0), dx_s.at[s], dx_r.at[s], (d, xn))

    def dy_copy(s):
        return remote(half(s, xn, 1), half(s, xn, 1), dy_s.at[s], dy_r.at[s], (d, yn))

    def hp_copy(src, s, mm, k):
        return remote(src, spot(s, mm), hp_s.at[s, k], hp_r.at[s, k], (d, pn))

    own = pltpu.make_async_copy(h_ref, spot(d, m), loc_sem.at[0])
    own.start()
    own_draft = pltpu.make_async_copy(draft_ref, dv.at[d], loc_sem.at[1])
    own_draft.start()

    @pl.when(d < NZ - 1)
    def _():
        hz_copy(h_ref, d, hz_s.at[d], d + 1).start()

    @pl.when(d > 0)
    def _():
        hz_copy(h_ref, d, hz_s.at[NZ], d - 1).start()

    hx_copy(h_ref, d).start()
    hy_copy(h_ref, d).start()
    hp_copy(h_ref, d, m, 0).start()
    drafts = [
        remote(draft_ref, dv.at[d], dr_s.at[j - 1], dr_r.at[j - 1], (lax.rem(d + j, NZ), m)) for j in (1, 2, 3)
    ]
    for copy in drafts:
        copy.start()

    spans = [(c * big, big) for c in range(count)] + [(count * big, tail)]
    to_near, from_near = 1 + 2 * (d % 2), 3 - 2 * (d % 2)

    def send_weights(lo, hi):
        for idx in range(lo, hi):
            for j in (2, 1, 3):
                w_copy(j, idx, *spans[idx]).start()

    for o in OFFSETS:
        s = d + o

        @pl.when((s >= 0) & (s < NZ))
        def _(o=o, s=s):
            src = spot(s, m)
            hz_copy(src, s, hz_s.at[s], d + (1 if o < 0 else -1)).wait_recv()
            if o < 0:
                @pl.when(d < NZ - 1)
                def _():
                    hz_copy(src, s, hz_s.at[s], d + 1).start()
            else:
                @pl.when(d > 0)
                def _():
                    hz_copy(src, s, hz_s.at[s], d - 1).start()
            hx_copy(src, s).start()
            hy_copy(src, s).start()
            hp_copy(src, s, m, 0).start()

        if o == 1:
            send_weights(0, 1)
            w_copy(to_near, count, *spans[count]).start()

            @pl.when((d == 0) | (d == NZ - 1))
            def _():
                for j in (2, from_near):
                    w_copy(j, count, *spans[count]).start()

        if o == 2:
            send_weights(1, count)

    for o in (0,) + OFFSETS:
        s = d + o

        @pl.when((s >= 0) & (s < NZ))
        def _(s=s):
            hx_copy(spot(s, m), s).wait_recv()
            dy_copy(s).start()
            hp_copy(spot(s, xn), s, xn, 1).start()
            hy_copy(spot(s, m), s).wait_recv()
            dx_copy(s).start()
            hp_copy(spot(s, yn), s, yn, 2).start()

    for o in (0,) + OFFSETS:
        s = d + o

        @pl.when((s >= 0) & (s < NZ))
        def _(s=s):
            dx_copy(s).wait_recv()
            dy_copy(s).wait_recv()
            hp_copy(spot(s, xy), s, xy, 3).start()

    m_acc[...] = jnp.full(m_acc.shape, -jnp.inf, jnp.float32)
    s_acc[...] = jnp.zeros_like(s_acc)
    p_acc[...] = jnp.zeros_like(p_acc)

    own.wait()
    own_draft.wait()
    for copy in drafts:
        copy.wait()
    for s in range(NZ):
        for k in range(4):
            hp_copy(spot(s, m), s, m, k).wait_recv()

    base = m * shard + piece_start(d)
    limit = step + (piece - step) * (d // 2)

    per = slab // BLOCK
    blocks = NZ * per
    hw = 2 * width
    near = pl.ds(pl.multiple_of(d // 2 * hw, hw), hw)

    def load(src, c0, size, cols, k):
        return pltpu.make_async_copy(src.at[pl.ds(pl.multiple_of(c0, 16), size), cols], wb.at[pl.ds(0, size), cols], ld_sem.at[k])

    def load_own(c0, size):
        cols = pl.ds(pl.multiple_of(d * width, width), width)
        return pltpu.make_async_copy(
            w_ref.at[pl.ds(pl.multiple_of(piece_start(d) + c0, 16), size), :], wb.at[pl.ds(0, size), cols], ld_sem.at[0]
        )

    def column(j):
        return pl.ds(pl.multiple_of(lax.rem(d + NZ - j, NZ) * width, width), width)

    from_inner = lax.rem(d + NZ - (2 - d // 2), NZ)
    from_outer = lax.rem(d + NZ - (3 - 3 * (d // 2)), NZ)

    def block_of(n):
        return pl.ds(pl.multiple_of(n * BLOCK, BLOCK), BLOCK)

    def product(n, size, cols):
        return lax.dot_general(
            wb[pl.ds(0, size), cols], hv[block_of(n), cols], (((1,), (1,)), ((), ())), preferred_element_type=jnp.float32
        )

    def fold(n, c0, size, ref, last):
        cols = block_of(n)
        tiles = ref[pl.ds(0, size), :].reshape(size // 8, 8, BLOCK)
        ids = 8 * lax.broadcasted_iota(jnp.int32, tiles.shape, 0) + lax.broadcasted_iota(jnp.int32, tiles.shape, 1)
        want = dv[n // per, :, pl.ds(pl.multiple_of((n % per) * BLOCK, BLOCK), BLOCK)] - (base + c0)
        if last:
            tiles = jnp.where(ids < limit - c0, tiles, -jnp.inf)
            want = jnp.where(want < limit - c0, want, -1)
        old = m_acc[:, cols]
        new = jnp.maximum(old, jnp.max(tiles, axis=0))
        m_acc[:, cols] = new
        s_acc[:, cols] = s_acc[:, cols] * jnp.exp(old - new) + jnp.sum(jnp.exp(tiles - new[None]), axis=0)
        p_acc[:, cols] = p_acc[:, cols] + jnp.sum(jnp.where(ids == want[None], tiles, 0.0), axis=0)

    def sweep(c0, size, fill, last):
        def pair(n, carry):
            fill(2 * n + 1, odd)
            fold(2 * n, c0, size, even, last)
            fill(2 * n + 2, even)
            fold(2 * n + 1, c0, size, odd, last)
            return carry

        fill(0, even)
        lax.fori_loop(0, blocks // 2 - 1, pair, 0)
        fill(blocks - 1, odd)
        fold(blocks - 2, c0, size, even, last)
        fold(blocks - 1, c0, size, odd, last)

    t0 = count * big
    loads = [load_own(t0, tail)]
    for k, j in enumerate((from_near, from_outer)):
        w_copy(j, count, t0, tail).wait_recv()
        loads.append(load(land_ref, t0, tail, column(j), 1 + k))
    for copy in loads:
        copy.start()
    for copy in loads:
        copy.wait()

    def first_half(n, carry):
        part_acc[:, block_of(n)] = product(n, tail, near) + product(n, tail, column(from_outer))
        return carry

    lax.fori_loop(0, blocks, first_half, 0)

    def big_chunk(c, carry):
        c0 = c * big
        loads = [load_own(c0, big)]
        loads[0].start()
        for j in (1, 2, 3):
            w_copy(j, c, c0, big).wait_recv()
            loads.append(load(land_ref, c0, big, column(j), j))
            loads[-1].start()

        @pl.when((c + LATE == count) & (d > 0) & (d < NZ - 1))
        def _():
            for j in (2, from_near):
                w_copy(j, count, t0, tail).start()

        for copy in loads:
            copy.wait()

        def fill(n, ref):
            ref[...] = product(n, big, slice(None))

        sweep(c0, big, fill, False)
        return carry

    lax.fori_loop(0, count, big_chunk, 0)

    w_copy(from_inner, count, t0, tail).wait_recv()
    rest = load(land_ref, t0, tail, column(from_inner), 1)
    rest.start()
    rest.wait()

    def fill_rest(n, ref):
        ref[pl.ds(0, tail), :] = part_acc[:, block_of(n)] + product(n, tail, column(from_inner))

    sweep(t0, tail, fill_rest, True)

    def put(ref, at, *share):
        for k, value in enumerate(share):
            ref[at, :, pl.ds(k * slab, slab)] = value

    for t in range(NZ):
        cols = pl.ds(t * slab, slab)
        tops = m_acc[:, cols]
        top = jnp.max(tops, axis=0, keepdims=True)
        total = jnp.sum(s_acc[:, cols] * jnp.exp(tops - top), axis=0, keepdims=True)
        put(stats, t, top + jnp.log(total), jnp.sum(p_acc[:, cols], axis=0, keepdims=True))

    for idx, span in enumerate(spans):
        for j in (1, 2, 3):
            w_copy(j, idx, *span).wait_send()

    @pl.when(d < NZ - 1)
    def _():
        hz_copy(h_ref, d, hz_s.at[d], d + 1).wait_send()

    @pl.when(d > 0)
    def _():
        hz_copy(h_ref, d, hz_s.at[NZ], d - 1).wait_send()

    for o in OFFSETS:
        s = d + o
        on = (s >= 0) & (d < NZ - 1) if o < 0 else (s < NZ) & (d > 0)

        @pl.when(on)
        def _(o=o, s=s):
            hz_copy(spot(s, m), s, hz_s.at[s], d + (1 if o < 0 else -1)).wait_send()

    for s in range(NZ):
        hx_copy(spot(s, m), s).wait_send()
        hy_copy(spot(s, m), s).wait_send()
        dx_copy(s).wait_send()
        dy_copy(s).wait_send()
        for k in range(4):
            hp_copy(spot(s, m), s, m, k).wait_send()

    def zx_copy(j):
        t = lax.rem(d + j, NZ)
        return remote(stats.at[t], zin.at[j - 1], zx_s.at[j - 1], zx_r.at[j - 1], (t, m))

    def mx_copy(k):
        return remote(gat.at[m], gat.at[m], mx_s.at[k - 1], mx_r.at[k - 1], (d, lax.rem(m + k, NM)))

    for j in (2, 1, 3):
        zx_copy(j).start()
    for j in (1, 2, 3):
        zx_copy(j).wait()
    shares = [stats[d]] + [zin[j] for j in range(NZ - 1)]
    put(gat, m, *merge(shares))
    for k in range(1, NM):
        mx_copy(k).start()
    for k in range(1, NM):
        mx_copy(k).wait()
    lse, picked = merge([gat[k] for k in range(NM)])
    log_prob = picked - lse
    logp_ref[...] = log_prob
    accept_ref[...] = jnp.minimum(1.0, jnp.exp(log_prob) / q_ref[...])


def solution(mesh):
    def per_device(h_part, w_part, draft_loc, q_loc):
        slab, part = h_part.shape
        shard, width = w_part.shape
        rows, full = slab * NZ, part * NM
        step = shard // NZ // 16 * 16
        piece = shard - 3 * step - ((shard - 3 * step) - step) // 2
        big, count = BIG, (piece - 1) // BIG
        n_chunks = count + 1
        cfg = (slab, part, piece, step, shard, width, big, count)
        dma = pltpu.SemaphoreType.DMA
        log_prob, accept, _ = pl.pallas_call(
            functools.partial(kernel, cfg),
            out_shape=(
                jax.ShapeDtypeStruct((1, slab), jnp.float32),
                jax.ShapeDtypeStruct((1, slab), jnp.float32),
                jax.ShapeDtypeStruct((piece, full), jnp.bfloat16),
            ),
            in_specs=[pl.BlockSpec(memory_space=pl.ANY)] * 3 + [pl.BlockSpec(memory_space=pltpu.VMEM)],
            out_specs=(
                pl.BlockSpec(memory_space=pltpu.VMEM),
                pl.BlockSpec(memory_space=pltpu.VMEM),
                pl.BlockSpec(memory_space=pl.ANY),
            ),
            scratch_shapes=[
                pltpu.VMEM((rows, full), jnp.bfloat16),
                pltpu.VMEM((big, full), jnp.bfloat16),
                pltpu.VMEM((NZ, 1, slab), jnp.int32),
                pltpu.VMEM((8, rows), jnp.float32),
                pltpu.VMEM((8, rows), jnp.float32),
                pltpu.VMEM((8, rows), jnp.float32),
                pltpu.VMEM((big, BLOCK), jnp.float32),
                pltpu.VMEM((big, BLOCK), jnp.float32),
                pltpu.VMEM((piece - count * big, rows), jnp.float32),
                pltpu.VMEM((NZ, 1, 2 * slab), jnp.float32),
                pltpu.VMEM((NZ - 1, 1, 2 * slab), jnp.float32),
                pltpu.VMEM((NM, 1, 2 * slab), jnp.float32),
                dma((NZ - 1,)), dma((NZ - 1,)), dma((NM - 1,)), dma((NM - 1,)),
                dma((2,)), dma((3,)), dma((3,)), dma((NZ + 1,)), dma((NZ,)),
                dma((NZ,)), dma((NZ,)), dma((NZ,)), dma((NZ,)),
                dma((NZ,)), dma((NZ,)), dma((NZ,)), dma((NZ,)),
                dma((NZ, 4)), dma((NZ, 4)), dma((3, n_chunks)), dma((3, n_chunks)), dma((4,)),
            ],
            compiler_params=pltpu.CompilerParams(
                collective_id=0, has_side_effects=True, vmem_limit_bytes=67043328
            ),
        )(h_part, w_part, draft_loc.reshape(1, slab), q_loc.reshape(1, slab))
        return log_prob.reshape(slab), accept.reshape(slab)

    return jax.shard_map(per_device, mesh=mesh, in_specs=(P("data", "model"), P("model", "data"), P("data"), P("data")), out_specs=(P("data"), P("data")), check_vma=False)
```
